32 devices in a mesh: dp: 2 (over x), row: 4 (over y, core), col: 4 (over z).
Axes of the slice: x: 2, y: 2, z: 4, core: 2. Of those that a mesh axis runs over, the one named last changes fastest.
Arguments:
- latents: float32 [24, 32, 128], P(('dp', 'row')), may hold values from -6 to 6
- labels: int32 [24], P(('dp', 'row')), may hold values from 0 to 999
- step_index: int32 [24], P(('dp', 'row')), may hold values from 1 to 8
- seeds: int32 [24], P(('dp', 'row')), may hold values from 0 to 2147483646
- class_table: bfloat16 [1000, 1152], replicated, may hold values from -6 to 6
- teacher_patch: bfloat16 [16, 1152], replicated, may hold values from -1.5 to 1.5
- teacher_mod: bfloat16 [1152, 3, 1152], P(('dp', 'row'), None, 'col'), may hold values from -0.1875 to 0.1875
- teacher_up: bfloat16 [1152, 4608], P(('dp', 'row'), 'col'), may hold values from -0.1875 to 0.1875
- teacher_down: bfloat16 [1152, 4608], P(('dp', 'row'), 'col'), may hold values from -0.09375 to 0.09375
- teacher_out: bfloat16 [16, 1152], replicated, may hold values from -0.1875 to 0.1875
- student_patch: bfloat16 [16, 1152], replicated, may hold values from -1.5 to 1.5
- student_mod: bfloat16 [1152, 3, 1152], P(('dp', 'row'), None, 'col'), may hold values from -0.1875 to 0.1875
- student_up: bfloat16 [1152, 4608], P(('dp', 'row'), 'col'), may hold values from -0.1875 to 0.1875
- student_down: bfloat16 [1152, 4608], P(('dp', 'row'), 'col'), may hold values from -0.09375 to 0.09375
- student_out: bfloat16 [16, 1152], replicated, may hold values from -0.1875 to 0.1875
Outputs:
- up_gradient: float32 [1152, 4608], P(('dp', 'row'), 'col')
- down_gradient: float32 [1152, 4608], P(('dp', 'row'), 'col')
The draws below stay inside these ranges and needn't reach their ends.
All inputs are finite; a program needn't handle non-finite values.
Results may differ from the reference program's by a relative error of at most 0.002.
Values may be sent and summed in bfloat16 or wider, within the bound.
A program may use at most 128 MiB of HBM per device.

```python
import math
import jax
import jax.numpy as jnp
from jax import lax

D = 1152
FF = 4608
CLASSES = 1000
SEQ = 256
PATCH = 16
STEPS = 8
BATCH = 24
N_COL = 4


def touch_ends(values, own_key, smallest, high):
    shape = values.shape
    spot = [jax.random.randint(jax.random.fold_in(own_key, axis), (), 0, shape[axis]) for axis in range(len(shape))]
    values = values.at[tuple(spot)].set(smallest)
    longest = shape.index(max(shape))
    spot[longest] = (spot[longest] + 1) % shape[longest]
    return values.at[tuple(spot)].set(high)


def levels(own_key, shape, shards, least, high):
    gain, own = 1.0, jax.random.fold_in(own_key, 6)
    for dim, shards_of in shards:
        draws = jnp.exp(jax.random.uniform(jax.random.fold_in(own, dim), (shards_of,), jnp.float32, least / len(shards), high / len(shards)))
        gain = gain * jnp.repeat(draws, shape[dim] // shards_of).reshape([-1 if axis == dim else 1 for axis in range(len(shape))])
    return gain


def gaussian(stream_key, shape, deviation, reach, split=(), held_as=jnp.bfloat16):
    entries = deviation * jax.random.normal(stream_key, shape, jnp.float32)
    if split:
        entries = entries * levels(stream_key, shape, split, -0.22, 0.18)
    return jnp.clip(entries, -reach, reach).astype(held_as)


def setup_inputs(seed: int = 0) -> dict:
    streams_of = jax.random.split(jax.random.key(seed), 16)
    return {
        "latents": gaussian(streams_of[0], (BATCH, SEQ * PATCH // 128, 128), 1.0, 6.0, ((0, 8),), jnp.float32),
        "labels": touch_ends(jax.random.randint(streams_of[1], (BATCH,), 0, CLASSES), jax.random.fold_in(streams_of[1], 1), 0, CLASSES - 1).astype(jnp.int32),
        "step_index": touch_ends(jax.random.randint(streams_of[2], (BATCH,), 1, STEPS + 1), jax.random.fold_in(streams_of[2], 1), 1, STEPS).astype(jnp.int32),
        "seeds": touch_ends(jax.random.randint(streams_of[3], (BATCH,), 0, 2147483647), jax.random.fold_in(streams_of[3], 1), 0, 2147483646).astype(jnp.int32),
        "class_table": gaussian(streams_of[4], (CLASSES, D), 1.0, 6.0),
        "teacher_patch": gaussian(streams_of[5], (PATCH, D), PATCH ** -0.5, 1.5),
        "teacher_mod": gaussian(streams_of[6], (D, 3, D), D ** -0.5, 0.1875, ((0, 8), (2, 4))),
        "teacher_up": gaussian(streams_of[7], (D, FF), D ** -0.5, 0.1875, ((0, 8), (1, 4))),
        "teacher_down": gaussian(streams_of[8], (D, FF), FF ** -0.5, 0.09375, ((0, 8), (1, 4))),
        "teacher_out": gaussian(streams_of[9], (PATCH, D), D ** -0.5, 0.1875),
        "student_patch": gaussian(streams_of[10], (PATCH, D), PATCH ** -0.5, 1.5),
        "student_mod": gaussian(streams_of[11], (D, 3, D), D ** -0.5, 0.1875, ((0, 8), (2, 4))),
        "student_up": gaussian(streams_of[12], (D, FF), D ** -0.5, 0.1875, ((0, 8), (1, 4))),
        "student_down": gaussian(streams_of[13], (D, FF), FF ** -0.5, 0.09375, ((0, 8), (1, 4))),
        "student_out": gaussian(streams_of[14], (PATCH, D), D ** -0.5, 0.1875),
    }


HALF_PI = 0.5 * math.pi
ROOT_TWO_PI = math.sqrt(2.0 / math.pi)

def plan(times):
    return (jnp.cos(HALF_PI * times), jnp.sin(HALF_PI * times))

def mixing(value):
    amount = jnp.int32(16)
    value = value ^ lax.shift_right_logical(value, amount)
    value = value * 73244475
    value = value ^ lax.shift_right_logical(value, amount)
    value = value * 73244475
    value = value ^ lax.shift_right_logical(value, amount)
    return value

def noise_of(seeds):
    total = SEQ * PATCH
    places = jnp.arange(total, dtype=jnp.int32).reshape(1, total // 128, 128)
    mixed = mixing(seeds[:, None, None] * 1103515245 + places * 40503 + 12345)
    uniform = (lax.shift_right_logical(mixed, jnp.int32(8)).astype(jnp.float32) + 0.5) * (1.0 / 16777216.0)
    return math.sqrt(2.0) * lax.erf_inv(2.0 * uniform - 1.0)

def time_features(times):
    half = D // 2
    freqs = jnp.exp(-math.log(10000.0) * jnp.arange(half, dtype=jnp.float32) / half)
    angle = (1000.0 * times)[:, None] * freqs[None, :]
    return jnp.concatenate([jnp.cos(angle), jnp.sin(angle)], axis=1)

def condition(times, labels, class_table):
    onehot = (labels[:, None] == jnp.arange(CLASSES, dtype=jnp.int32)[None, :]).astype(jnp.bfloat16)
    embedded = jnp.dot(onehot, class_table, preferred_element_type=jnp.float32)
    return jax.nn.silu(embedded + time_features(times)).astype(jnp.bfloat16)

def modulation(cond, weight):
    return jnp.einsum('nd,dkf->nkf', cond.astype(jnp.float32), weight.astype(jnp.float32), precision=lax.Precision.HIGHEST)

def positions():
    quarter = D // 4
    omega = 1.0 / 10000.0 ** (jnp.arange(quarter, dtype=jnp.float32) / quarter)
    side = math.isqrt(SEQ)
    cells = jnp.arange(SEQ, dtype=jnp.int32)
    grid_row = (cells // side).astype(jnp.float32)
    grid_col = (cells % side).astype(jnp.float32)
    row_angle = grid_row[:, None] * omega[None, :]
    col_angle = grid_col[:, None] * omega[None, :]
    return jnp.concatenate([jnp.sin(row_angle), jnp.cos(row_angle), jnp.sin(col_angle), jnp.cos(col_angle)], axis=1)

def layer_norm(values):
    center = values - lax.optimization_barrier(jnp.mean(values, axis=-1, keepdims=True))
    spread = lax.optimization_barrier(jnp.mean(center * center, axis=-1, keepdims=True))
    reciprocal = lax.rsqrt(spread + 1e-06)
    return (center * reciprocal, reciprocal)

def gelu_slope(pre):
    inner = ROOT_TWO_PI * (pre + 0.044715 * pre * pre * pre)
    tangent = jnp.tanh(inner)
    return 0.5 * (1.0 + tangent) + 0.5 * pre * (1.0 - tangent * tangent) * ROOT_TWO_PI * (1.0 + 3.0 * 0.044715 * pre * pre)

def contract_last(left, right):
    return lax.dot_general(left, right, (((1,), (1,)), ((), ())), preferred_element_type=jnp.float32)

def contract_first(left, right):
    return lax.dot_general(left, right, (((0,), (0,)), ((), ())), preferred_element_type=jnp.float32)

def network(state, mods, patch_weight, up_weight, down_weight, out_weight, pos):
    samples = state.shape[0]
    tokens = state.reshape(samples * SEQ, PATCH).astype(jnp.bfloat16)
    base = jnp.dot(tokens, patch_weight, preferred_element_type=jnp.float32).reshape(samples, SEQ, D) + pos[None]
    shift = mods[:, 0][:, None, :]
    scale = mods[:, 1][:, None, :]
    gate = mods[:, 2][:, None, :]
    normed, _ = layer_norm(base)
    act = (normed * (1.0 + scale) + shift).astype(jnp.bfloat16).reshape(samples * SEQ, D)
    pre = jnp.dot(act, up_weight, preferred_element_type=jnp.float32)
    hidden = jax.nn.gelu(pre, approximate=True).astype(jnp.bfloat16)
    width = FF // N_COL
    mixed = jnp.zeros((samples * SEQ, D), jnp.float32)
    for column in range(N_COL):
        part = contract_last(hidden[:, column * width:(column + 1) * width], down_weight[:, column * width:(column + 1) * width])
        rounded = lax.optimization_barrier(part.astype(jnp.bfloat16))
        mixed = mixed + rounded.astype(jnp.float32)
    later = base + gate * mixed.reshape(samples, SEQ, D)
    final, reciprocal = layer_norm(later)
    velocity = contract_last(final.astype(jnp.bfloat16).reshape(samples * SEQ, D), out_weight)
    return (velocity.reshape(samples, SEQ * PATCH // 128, 128), (act, pre, hidden, final, reciprocal, gate))

def reference(latents, labels, step_index, seeds, class_table, teacher_patch, teacher_mod, teacher_up, teacher_down, teacher_out, student_patch, student_mod, student_up, student_down, student_out):
    block = 8
    count = BATCH // block
    pos = positions()

    def one_block(carry, inputs):
        clean, names, steps, keys = inputs
        now = steps.astype(jnp.float32) / STEPS
        middle = now - 0.5 / STEPS
        ending = now - 1.0 / STEPS
        alpha, sigma = plan(now[:, None, None])
        alpha_mid, sigma_mid = plan(middle[:, None, None])
        alpha_end, sigma_end = plan(ending[:, None, None])
        cond_now = condition(now, names, class_table)
        cond_mid = condition(middle, names, class_table)
        teacher_now = modulation(cond_now, teacher_mod)
        teacher_mid = modulation(cond_mid, teacher_mod)
        student_mods = modulation(cond_now, student_mod)
        noisy = alpha * clean + sigma * noise_of(keys)
        first_v, _ = network(noisy, teacher_now, teacher_patch, teacher_up, teacher_down, teacher_out, pos)
        first_x = alpha * noisy - sigma * first_v
        halfway = alpha_mid * first_x + sigma_mid * (noisy - alpha * first_x) / sigma
        second_v, _ = network(halfway, teacher_mid, teacher_patch, teacher_up, teacher_down, teacher_out, pos)
        second_x = alpha_mid * halfway - sigma_mid * second_v
        landing = alpha_end * second_x + sigma_end * (halfway - alpha_mid * second_x) / sigma_mid
        ratio = sigma_end / sigma
        target = (landing - ratio * noisy) / (alpha_end - ratio * alpha)
        student_v, saved = network(noisy, student_mods, student_patch, student_up, student_down, student_out, pos)
        student_x = alpha * noisy - sigma * student_v
        weight = jnp.maximum(alpha * alpha / (sigma * sigma), 1.0)
        back_velocity = (-2.0 * sigma * weight * (student_x - target) / BATCH).reshape(block * SEQ, PATCH)
        act, pre, hidden, final, reciprocal, gate = saved
        back_final = jnp.dot(back_velocity, student_out.astype(jnp.float32), precision=lax.Precision.HIGHEST).reshape(block, SEQ, D)
        centre = lax.optimization_barrier(jnp.mean(back_final, axis=2, keepdims=True))
        along = lax.optimization_barrier(jnp.mean(back_final * final, axis=2, keepdims=True))
        back_mixed = (gate * (reciprocal * (back_final - centre - final * along))).astype(jnp.bfloat16).reshape(block * SEQ, D)
        down_term = contract_first(back_mixed, hidden)
        back_hidden = jnp.dot(back_mixed, student_down, preferred_element_type=jnp.float32)
        back_pre = (back_hidden * gelu_slope(pre)).astype(jnp.bfloat16)
        up_term = contract_first(act, back_pre)
        return ((carry[0] + up_term, carry[1] + down_term), None)
    inputs = (latents.reshape(count, block, SEQ * PATCH // 128, 128), labels.reshape(count, block), step_index.reshape(count, block), seeds.reshape(count, block))
    zeros = jnp.zeros((D, FF), jnp.float32)
    (up_gradient, down_gradient), _ = lax.scan(one_block, (zeros, zeros), inputs)
    return (up_gradient, down_gradient)
```

```python
import math

import jax
import jax.numpy as jnp
from jax import lax
from jax.sharding import PartitionSpec as P

D = 1152
CLASSES = 1000
SEQ = 256
PATCH = 16
STEPS = 8


HALF_PI = 0.5 * math.pi
ROOT_TWO_PI = math.sqrt(2.0 / math.pi)


def plan(times):
    return (jnp.cos(HALF_PI * times), jnp.sin(HALF_PI * times))


def mixing(value):
    amount = jnp.int32(16)
    value = value ^ lax.shift_right_logical(value, amount)
    value = value * 73244475
    value = value ^ lax.shift_right_logical(value, amount)
    value = value * 73244475
    value = value ^ lax.shift_right_logical(value, amount)
    return value


def noise_of(seeds):
    total = SEQ * PATCH
    places = jnp.arange(total, dtype=jnp.int32).reshape(1, total // 128, 128)
    mixed = mixing(seeds[:, None, None] * 1103515245 + places * 40503 + 12345)
    uniform = (lax.shift_right_logical(mixed, jnp.int32(8)).astype(jnp.float32) + 0.5) * (
        1.0 / 16777216.0
    )
    return math.sqrt(2.0) * lax.erf_inv(2.0 * uniform - 1.0)


def time_features(times):
    half = D // 2
    freqs = jnp.exp(-math.log(10000.0) * jnp.arange(half, dtype=jnp.float32) / half)
    angle = (1000.0 * times)[:, None] * freqs[None, :]
    return jnp.concatenate([jnp.cos(angle), jnp.sin(angle)], axis=1)


def condition(times, labels, class_table):
    onehot = (labels[:, None] == jnp.arange(CLASSES, dtype=jnp.int32)[None, :]).astype(jnp.bfloat16)
    embedded = jnp.dot(onehot, class_table, preferred_element_type=jnp.float32)
    return jax.nn.silu(embedded + time_features(times)).astype(jnp.bfloat16)


def positions():
    quarter = D // 4
    omega = 1.0 / 10000.0 ** (jnp.arange(quarter, dtype=jnp.float32) / quarter)
    side = math.isqrt(SEQ)
    cells = jnp.arange(SEQ, dtype=jnp.int32)
    grid_row = (cells // side).astype(jnp.float32)
    grid_col = (cells % side).astype(jnp.float32)
    row_angle = grid_row[:, None] * omega[None, :]
    col_angle = grid_col[:, None] * omega[None, :]
    return jnp.concatenate(
        [jnp.sin(row_angle), jnp.cos(row_angle), jnp.sin(col_angle), jnp.cos(col_angle)], axis=1
    )


def layer_norm(values):
    center = values - jnp.mean(values, axis=-1, keepdims=True)
    spread = jnp.mean(center * center, axis=-1, keepdims=True)
    reciprocal = lax.rsqrt(spread + 1e-06)
    return (center * reciprocal, reciprocal)


def gelu_slope(pre):
    inner = ROOT_TWO_PI * (pre + 0.044715 * pre * pre * pre)
    tangent = jnp.tanh(inner)
    return 0.5 * (1.0 + tangent) + 0.5 * pre * (1.0 - tangent * tangent) * ROOT_TWO_PI * (
        1.0 + 3.0 * 0.044715 * pre * pre
    )


def contract_last(left, right):
    return lax.dot_general(
        left, right, (((1,), (1,)), ((), ())), preferred_element_type=jnp.float32
    )


def contract_first(left, right):
    return lax.dot_general(
        left, right, (((0,), (0,)), ((), ())), preferred_element_type=jnp.float32
    )


def modulate(base, mods):
    normed, _ = layer_norm(base)
    shift = mods[:, 0][None, :, None, :]
    scale = mods[:, 1][None, :, None, :]
    return (normed * (1.0 + scale) + shift).astype(jnp.bfloat16).reshape(-1, D)


def embed(tokens, patch_weight, pos):
    flat = tokens.reshape(-1, PATCH)
    product = jnp.dot(flat, patch_weight, preferred_element_type=jnp.float32)
    return product.reshape(*tokens.shape[:-1], D) + pos


def scatter_columns(partial_out, groups):
    blocks = partial_out.reshape(groups, -1, D)
    swapped = lax.all_to_all(blocks, "col", split_axis=0, concat_axis=0, tiled=True)
    return jnp.sum(swapped.astype(jnp.float32), axis=0)


def reduce_gradient(left, right, group):
    partial = contract_first(left, right).astype(jnp.bfloat16)
    blocks = partial.reshape(group, partial.shape[0] // group, partial.shape[1])
    swapped = lax.all_to_all(blocks, ("dp", "row"), split_axis=0, concat_axis=0, tiled=True)
    return jnp.sum(swapped.astype(jnp.float32), axis=0)


def body(
    latents,
    labels,
    step_index,
    seeds,
    class_table,
    teacher_patch,
    teacher_mod,
    teacher_up,
    teacher_down,
    teacher_out,
    student_patch,
    student_mod,
    student_up,
    student_down,
    student_out,
):
    samples = latents.shape[0]
    group = lax.axis_size(("dp", "row"))
    groups = lax.axis_size("col")
    column = lax.axis_index("col")
    chunk = SEQ // groups
    batch_total = samples * group
    up_panel, down_panel, student_up_panel, student_panel = [
        lax.all_gather(weight, ("dp", "row"), axis=0, tiled=True)
        for weight in (teacher_up, teacher_down, student_up, student_down)
    ]
    both = lax.all_gather(jnp.stack([labels, step_index]), ("dp", "row"), axis=1, tiled=True)
    all_labels, all_steps = both[0], both[1]
    all_now = all_steps.astype(jnp.float32) / STEPS
    cond = condition(
        jnp.concatenate([all_now, all_now - 0.5 / STEPS]),
        jnp.concatenate([all_labels, all_labels]),
        class_table,
    )
    own_rows = teacher_mod.shape[0]
    offset = lax.axis_index(("dp", "row")) * own_rows
    rows = lax.dynamic_slice_in_dim(cond, offset, own_rows, 1)
    width = teacher_mod.shape[2]
    teacher_part = jnp.dot(
        rows, teacher_mod.reshape(own_rows, 3 * width), preferred_element_type=jnp.float32
    ).reshape(2, batch_total, 3 * width)
    student_part = jnp.dot(
        rows[:batch_total],
        student_mod.reshape(own_rows, 3 * width),
        preferred_element_type=jnp.float32,
    )[None]
    parts = jnp.concatenate([teacher_part, student_part], axis=0)
    parts = parts.reshape(3, group, samples, 3 * width).transpose(1, 0, 2, 3)
    parts = parts.reshape(group, 3 * samples, 3 * width)
    swapped = lax.all_to_all(parts, ("dp", "row"), split_axis=0, concat_axis=0, tiled=True)
    sums = jnp.sum(swapped, axis=0)
    mods = lax.all_gather(sums, "col", axis=0, tiled=False)
    mods = mods.reshape(groups, 3, samples, 3, width).transpose(1, 2, 3, 0, 4)
    mods = mods.reshape(3, samples, 3, D)

    now = step_index.astype(jnp.float32) / STEPS
    alpha, sigma = plan(now[:, None, None])
    alpha_mid, sigma_mid = plan((now - 0.5 / STEPS)[:, None, None])
    alpha_end, sigma_end = plan((now - 1.0 / STEPS)[:, None, None])
    noisy_full = alpha * latents + sigma * noise_of(seeds)
    noisy_full = noisy_full.reshape(samples, groups, chunk, PATCH).transpose(1, 0, 2, 3)
    noisy = lax.dynamic_index_in_dim(noisy_full, column, 0, keepdims=False)
    noisy_tokens = noisy_full.astype(jnp.bfloat16)
    pos = positions().reshape(groups, 1, chunk, D)
    own_pos = lax.dynamic_index_in_dim(pos, column, 0, keepdims=True)

    def own_output(own_base, gate, mixed, out_weight):
        later = own_base[0] + gate[:, None, :] * mixed.reshape(samples, chunk, D)
        final, _ = layer_norm(later)
        velocity = contract_last(final.astype(jnp.bfloat16).reshape(-1, D), out_weight)
        return velocity.reshape(samples, chunk, PATCH)

    def teacher(tokens, own_tokens, these):
        act = modulate(embed(tokens, teacher_patch, pos), these)
        pre = jnp.dot(act, up_panel, preferred_element_type=jnp.float32)
        hidden = jax.nn.gelu(pre, approximate=True).astype(jnp.bfloat16)
        mixed = scatter_columns(contract_last(hidden, down_panel).astype(jnp.bfloat16), groups)
        own_base = embed(own_tokens[None], teacher_patch, own_pos)
        return own_output(own_base, these[:, 2], mixed, teacher_out)

    first_v = teacher(noisy_tokens, noisy.astype(jnp.bfloat16), mods[0])
    first_x = alpha * noisy - sigma * first_v
    halfway = alpha_mid * first_x + sigma_mid * (noisy - alpha * first_x) / sigma
    halfway_own = halfway.astype(jnp.bfloat16)
    halfway_tokens = lax.all_gather(halfway_own, "col", axis=0, tiled=False)
    second_v = teacher(halfway_tokens, halfway_own, mods[1])
    second_x = alpha_mid * halfway - sigma_mid * second_v
    landing = alpha_end * second_x + sigma_end * (halfway - alpha_mid * second_x) / sigma_mid
    ratio = sigma_end / sigma
    target = (landing - ratio * noisy) / (alpha_end - ratio * alpha)

    student_mods = mods[2]
    gate = student_mods[:, 2]
    base = embed(noisy_tokens, student_patch, pos)
    act = modulate(base, student_mods)
    pre = jnp.dot(act, student_up_panel, preferred_element_type=jnp.float32)
    hidden = jax.nn.gelu(pre, approximate=True).astype(jnp.bfloat16)
    own_mixed = scatter_columns(contract_last(hidden, student_panel).astype(jnp.bfloat16), groups)
    own_base = embed(noisy.astype(jnp.bfloat16)[None], student_patch, own_pos)[0]
    later = own_base + gate[:, None, :] * own_mixed.reshape(samples, chunk, D)
    final, reciprocal = layer_norm(later)
    student_v = contract_last(final.astype(jnp.bfloat16).reshape(-1, D), student_out)
    student_x = alpha * noisy - sigma * student_v.reshape(samples, chunk, PATCH)
    weight = jnp.maximum(alpha * alpha / (sigma * sigma), 1.0)
    back_velocity = -2.0 * sigma * weight * (student_x - target) / batch_total
    back_final = jnp.dot(
        back_velocity.reshape(-1, PATCH),
        student_out.astype(jnp.float32),
        precision=lax.Precision.HIGHEST,
    ).reshape(samples, chunk, D)
    centre = jnp.mean(back_final, axis=2, keepdims=True)
    along = jnp.mean(back_final * final, axis=2, keepdims=True)
    own_back = (
        gate[:, None, :] * (reciprocal * (back_final - centre - final * along))
    ).astype(jnp.bfloat16)
    back_mixed = lax.all_gather(own_back.reshape(-1, D), "col", axis=0, tiled=True)
    back_hidden = jnp.dot(back_mixed, student_panel, preferred_element_type=jnp.float32)
    back_pre = (back_hidden * gelu_slope(pre)).astype(jnp.bfloat16)
    down_gradient = reduce_gradient(back_mixed, hidden, group)
    up_gradient = reduce_gradient(act, back_pre, group)
    return (up_gradient, down_gradient)


def solution(mesh):
    placed = (
        P(("dp", "row"), None, None),
        P(("dp", "row")),
        P(("dp", "row")),
        P(("dp", "row")),
        P(),
        P(),
        P(("dp", "row"), None, "col"),
        P(("dp", "row"), "col"),
        P(("dp", "row"), "col"),
        P(),
        P(),
        P(("dp", "row"), None, "col"),
        P(("dp", "row"), "col"),
        P(("dp", "row"), "col"),
        P(),
    )
    return jax.shard_map(
        body,
        mesh=mesh,
        in_specs=placed,
        out_specs=(P(("dp", "row"), "col"), P(("dp", "row"), "col")),
        check_vma=False,
    )
```

```python
import math

import jax
import jax.numpy as jnp
from jax import lax
from jax.sharding import PartitionSpec as P

D = 1152
CLASSES = 1000
SEQ = 256
PATCH = 16
STEPS = 8


HALF_PI = 0.5 * math.pi
ROOT_TWO_PI = math.sqrt(2.0 / math.pi)


def plan(times):
    return (jnp.cos(HALF_PI * times), jnp.sin(HALF_PI * times))


def mixing(value):
    amount = jnp.int32(16)
    value = value ^ lax.shift_right_logical(value, amount)
    value = value * 73244475
    value = value ^ lax.shift_right_logical(value, amount)
    value = value * 73244475
    value = value ^ lax.shift_right_logical(value, amount)
    return value


def noise_of(seeds):
    total = SEQ * PATCH
    places = jnp.arange(total, dtype=jnp.int32).reshape(1, total // 128, 128)
    mixed = mixing(seeds[:, None, None] * 1103515245 + places * 40503 + 12345)
    uniform = (lax.shift_right_logical(mixed, jnp.int32(8)).astype(jnp.float32) + 0.5) * (
        1.0 / 16777216.0
    )
    return math.sqrt(2.0) * lax.erf_inv(2.0 * uniform - 1.0)


def time_features(times):
    half = D // 2
    freqs = jnp.exp(-math.log(10000.0) * jnp.arange(half, dtype=jnp.float32) / half)
    angle = (1000.0 * times)[:, None] * freqs[None, :]
    return jnp.concatenate([jnp.cos(angle), jnp.sin(angle)], axis=1)


def condition(times, labels, class_table):
    onehot = (labels[:, None] == jnp.arange(CLASSES, dtype=jnp.int32)[None, :]).astype(jnp.bfloat16)
    embedded = jnp.dot(onehot, class_table, preferred_element_type=jnp.float32)
    return jax.nn.silu(embedded + time_features(times)).astype(jnp.bfloat16)


def positions():
    quarter = D // 4
    omega = 1.0 / 10000.0 ** (jnp.arange(quarter, dtype=jnp.float32) / quarter)
    side = math.isqrt(SEQ)
    cells = jnp.arange(SEQ, dtype=jnp.int32)
    grid_row = (cells // side).astype(jnp.float32)
    grid_col = (cells % side).astype(jnp.float32)
    row_angle = grid_row[:, None] * omega[None, :]
    col_angle = grid_col[:, None] * omega[None, :]
    return jnp.concatenate(
        [jnp.sin(row_angle), jnp.cos(row_angle), jnp.sin(col_angle), jnp.cos(col_angle)], axis=1
    )


def layer_norm(values):
    center = values - jnp.mean(values, axis=-1, keepdims=True)
    spread = jnp.mean(center * center, axis=-1, keepdims=True)
    reciprocal = lax.rsqrt(spread + 1e-06)
    return (center * reciprocal, reciprocal)


def gelu_slope(pre):
    inner = ROOT_TWO_PI * (pre + 0.044715 * pre * pre * pre)
    tangent = jnp.tanh(inner)
    return 0.5 * (1.0 + tangent) + 0.5 * pre * (1.0 - tangent * tangent) * ROOT_TWO_PI * (
        1.0 + 3.0 * 0.044715 * pre * pre
    )


def contract_last(left, right):
    return lax.dot_general(
        left, right, (((1,), (1,)), ((), ())), preferred_element_type=jnp.float32
    )


def contract_first(left, right):
    return lax.dot_general(
        left, right, (((0,), (0,)), ((), ())), preferred_element_type=jnp.float32
    )


def modulate(base, mods):
    normed, _ = layer_norm(base)
    shift = mods[0][None, :, None, :]
    scale = mods[1][None, :, None, :]
    return (normed * (1.0 + scale) + shift).astype(jnp.bfloat16).reshape(-1, D)


def embed(tokens, patch_weight, pos):
    flat = tokens.reshape(-1, PATCH)
    product = jnp.dot(flat, patch_weight, preferred_element_type=jnp.float32)
    return product.reshape(*tokens.shape[:-1], D) + pos


def scatter_columns(partial_out, groups):
    blocks = partial_out.reshape(groups, -1, D)
    swapped = lax.all_to_all(blocks, "col", split_axis=0, concat_axis=0, tiled=True)
    return jnp.sum(swapped.astype(jnp.float32), axis=0)


def reduce_gradient(left, right, group):
    names = ("dp", "row")
    me = lax.axis_index(names)
    pairs = group // 2
    mine, parity = me // 2, me % 2
    partial = contract_first(left, right)
    blocks = partial.reshape(pairs, 2, partial.shape[0] // group, partial.shape[1])
    keep = lax.dynamic_index_in_dim(blocks, parity, 1, keepdims=False)
    give = lax.dynamic_index_in_dim(blocks.astype(jnp.bfloat16), 1 - parity, 1, keepdims=False)
    got = lax.ppermute(give, names, [(i, i ^ 1) for i in range(group)])
    pair = keep + got.astype(jnp.float32)
    sent = pair.astype(jnp.bfloat16)
    total = lax.dynamic_index_in_dim(pair, mine, 0, keepdims=False)
    for step in range(1, pairs):
        piece = lax.dynamic_index_in_dim(sent, (mine + step) % pairs, 0, keepdims=False)
        hop = [(i, (i + 2 * step) % group) for i in range(group)]
        total = total + lax.ppermute(piece, names, hop).astype(jnp.float32)
    return total


def body(
    latents,
    labels,
    step_index,
    seeds,
    class_table,
    teacher_patch,
    teacher_mod,
    teacher_up,
    teacher_down,
    teacher_out,
    student_patch,
    student_mod,
    student_up,
    student_down,
    student_out,
):
    samples = latents.shape[0]
    group = lax.axis_size(("dp", "row"))
    groups = lax.axis_size("col")
    column = lax.axis_index("col")
    chunk = SEQ // groups
    batch_total = samples * group
    up_panel, down_panel, student_up_panel, student_panel = [
        lax.all_gather(weight, ("dp", "row"), axis=0, tiled=True)
        for weight in (teacher_up, teacher_down, student_up, student_down)
    ]
    both = lax.all_gather(jnp.stack([labels, step_index]), ("dp", "row"), axis=1, tiled=True)
    all_labels, all_steps = both[0], both[1]
    all_now = all_steps.astype(jnp.float32) / STEPS
    cond = condition(
        jnp.concatenate([all_now, all_now - 0.5 / STEPS]),
        jnp.concatenate([all_labels, all_labels]),
        class_table,
    )
    own_rows = teacher_mod.shape[0]
    offset = lax.axis_index(("dp", "row")) * own_rows
    rows = lax.dynamic_slice_in_dim(cond, offset, own_rows, 1)
    width = teacher_mod.shape[2]
    parts = []
    for taken, weights in ((2, teacher_mod), (1, student_mod)):
        for index in range(3):
            product = jnp.dot(
                rows[: taken * batch_total],
                weights[:, index],
                preferred_element_type=jnp.float32,
            ).reshape(taken, group, samples, width)
            parts.extend(product[which] for which in range(taken))
    parts = jnp.concatenate(parts, axis=1)
    swapped = lax.all_to_all(parts, ("dp", "row"), split_axis=0, concat_axis=0, tiled=True)
    sums = jnp.sum(swapped, axis=0)
    gathered = lax.all_gather(sums, "col", axis=0, tiled=False)
    joined = jnp.concatenate([gathered[place] for place in range(groups)], axis=-1)

    def entry(place):
        return joined[place * samples : (place + 1) * samples]

    teacher_now = [entry(2 * index) for index in range(3)]
    teacher_mid = [entry(2 * index + 1) for index in range(3)]
    student_mods = [entry(6 + index) for index in range(3)]

    now = step_index.astype(jnp.float32) / STEPS
    alpha, sigma = plan(now[:, None, None])
    alpha_mid, sigma_mid = plan((now - 0.5 / STEPS)[:, None, None])
    alpha_end, sigma_end = plan((now - 1.0 / STEPS)[:, None, None])
    noisy_full = alpha * latents + sigma * noise_of(seeds)
    noisy_full = noisy_full.reshape(samples, groups, chunk, PATCH).transpose(1, 0, 2, 3)
    noisy = lax.dynamic_index_in_dim(noisy_full, column, 0, keepdims=False)
    noisy_tokens = noisy_full.astype(jnp.bfloat16)
    pos = positions().reshape(groups, 1, chunk, D)
    own_pos = lax.dynamic_index_in_dim(pos, column, 0, keepdims=True)

    def own_output(own_base, gate, mixed, out_weight):
        later = own_base[0] + gate[:, None, :] * mixed.reshape(samples, chunk, D)
        final, _ = layer_norm(later)
        velocity = contract_last(final.astype(jnp.bfloat16).reshape(-1, D), out_weight)
        return velocity.reshape(samples, chunk, PATCH)

    def teacher(tokens, own_tokens, these):
        act = modulate(embed(tokens, teacher_patch, pos), these)
        pre = jnp.dot(act, up_panel, preferred_element_type=jnp.float32)
        hidden = jax.nn.gelu(pre, approximate=True).astype(jnp.bfloat16)
        mixed = scatter_columns(contract_last(hidden, down_panel).astype(jnp.bfloat16), groups)
        own_base = embed(own_tokens[None], teacher_patch, own_pos)
        return own_output(own_base, these[2], mixed, teacher_out)

    first_v = teacher(noisy_tokens, noisy.astype(jnp.bfloat16), teacher_now)
    first_x = alpha * noisy - sigma * first_v
    halfway = alpha_mid * first_x + sigma_mid * (noisy - alpha * first_x) / sigma
    halfway_own = halfway.astype(jnp.bfloat16)
    halfway_tokens = lax.all_gather(halfway_own, "col", axis=0, tiled=False)
    gate = student_mods[2]
    base = embed(noisy_tokens, student_patch, pos)
    act = modulate(base, student_mods)
    pre = jnp.dot(act, student_up_panel, preferred_element_type=jnp.float32)
    hidden = jax.nn.gelu(pre, approximate=True).astype(jnp.bfloat16)
    hidden, halfway_tokens = lax.optimization_barrier((hidden, halfway_tokens))
    second_v = teacher(halfway_tokens, halfway_own, teacher_mid)
    second_x = alpha_mid * halfway - sigma_mid * second_v
    landing = alpha_end * second_x + sigma_end * (halfway - alpha_mid * second_x) / sigma_mid
    ratio = sigma_end / sigma
    target = (landing - ratio * noisy) / (alpha_end - ratio * alpha)

    own_mixed = scatter_columns(contract_last(hidden, student_panel).astype(jnp.bfloat16), groups)
    own_base = embed(noisy.astype(jnp.bfloat16)[None], student_patch, own_pos)[0]
    later = own_base + gate[:, None, :] * own_mixed.reshape(samples, chunk, D)
    final, reciprocal = layer_norm(later)
    student_v = contract_last(final.astype(jnp.bfloat16).reshape(-1, D), student_out)
    student_x = alpha * noisy - sigma * student_v.reshape(samples, chunk, PATCH)
    weight = jnp.maximum(alpha * alpha / (sigma * sigma), 1.0)
    back_velocity = -2.0 * sigma * weight * (student_x - target) / batch_total
    back_final = jnp.dot(
        back_velocity.reshape(-1, PATCH),
        student_out.astype(jnp.float32),
        precision=lax.Precision.HIGHEST,
    ).reshape(samples, chunk, D)
    centre = jnp.mean(back_final, axis=2, keepdims=True)
    along = jnp.mean(back_final * final, axis=2, keepdims=True)
    own_back = (
        gate[:, None, :] * (reciprocal * (back_final - centre - final * along))
    ).astype(jnp.bfloat16)
    back_mixed = lax.all_gather(own_back.reshape(-1, D), "col", axis=0, tiled=True)
    back_hidden = jnp.dot(back_mixed, student_panel, preferred_element_type=jnp.float32)
    back_pre = (back_hidden * gelu_slope(pre)).astype(jnp.bfloat16)
    down_gradient = reduce_gradient(back_mixed, hidden, group)
    up_gradient = reduce_gradient(act, back_pre, group)
    return (up_gradient, down_gradient)


def solution(mesh):
    placed = (
        P(("dp", "row"), None, None),
        P(("dp", "row")),
        P(("dp", "row")),
        P(("dp", "row")),
        P(),
        P(),
        P(("dp", "row"), None, "col"),
        P(("dp", "row"), "col"),
        P(("dp", "row"), "col"),
        P(),
        P(),
        P(("dp", "row"), None, "col"),
        P(("dp", "row"), "col"),
        P(("dp", "row"), "col"),
        P(),
    )
    return jax.shard_map(
        body,
        mesh=mesh,
        in_specs=placed,
        out_specs=(P(("dp", "row"), "col"), P(("dp", "row"), "col")),
        check_vma=False,
    )
```
